32 devices in a mesh: img: 8 (over z, y), tile: 4 (over x, core).
Axes of the slice: x: 2, y: 2, z: 4, core: 2. Of those that a mesh axis runs over, the one named last changes fastest.
Arguments:
- tokens: bfloat16 [24, 4, 144, 768], P('img', 'tile'), may hold values from -6 to 6
- qkv_weight: bfloat16 [768, 2304], P(('img', 'tile')), may hold values from -0.21875 to 0.21875
- proj_weight: bfloat16 [768, 768], P(('img', 'tile')), may hold values from -0.875 to 0.875
- expand_weight: bfloat16 [768, 3072], P(('img', 'tile')), may hold values from -0.21875 to 0.21875
- reduce_weight: bfloat16 [3072, 768], P(('img', 'tile')), may hold values from -0.109375 to 0.109375
- qkv_down: bfloat16 [768, 128], P(('img', 'tile')), may hold values from -0.21875 to 0.21875
- qkv_up: bfloat16 [128, 2304], P(None, ('img', 'tile')), may hold values from -1.5 to 1.5
- proj_down: bfloat16 [768, 128], P(('img', 'tile')), may hold values from -0.21875 to 0.21875
- proj_up: bfloat16 [128, 768], P(None, ('img', 'tile')), may hold values from -1.5 to 1.5
- expand_down: bfloat16 [768, 128], P(('img', 'tile')), may hold values from -0.21875 to 0.21875
- expand_up: bfloat16 [128, 3072], P(None, ('img', 'tile')), may hold values from -1.5 to 1.5
- reduce_down: bfloat16 [3072, 128], P(('img', 'tile')), may hold values from -0.109375 to 0.109375
- reduce_up: bfloat16 [128, 768], P(None, ('img', 'tile')), may hold values from -1.5 to 1.5
- norm1_gain: float32 [768], replicated, may hold values from 0.5 to 1.5
- norm1_bias: float32 [768], replicated, may hold values from -3 to 3
- norm2_gain: float32 [768], replicated, may hold values from 0.5 to 1.5
- norm2_bias: float32 [768], replicated, may hold values from -3 to 3
- qkv_bias: float32 [2304], replicated, may hold values from -3 to 3
- proj_bias: float32 [768], replicated, may hold values from -3 to 3
- expand_bias: float32 [3072], replicated, may hold values from -3 to 3
- reduce_bias: float32 [768], replicated, may hold values from -3 to 3
- rel_table: float32 [529, 24], replicated, may hold values from -4 to 4
- slot_mask: int32 [24], P('img'), may hold values from 0 to 1, as said below
- adapter_index: int32 [24, 4], P('img'), may hold values from 0 to 7
- cotangent: bfloat16 [24, 4, 144, 768], P('img', 'tile'), may hold values from -6 to 6
Outputs:
- block_output: bfloat16 [24, 4, 144, 768], P('img', 'tile')
- input_grad: bfloat16 [24, 4, 144, 768], P('img', 'tile')
- qkv_down_grad: float32 [768, 128], P(('img', 'tile'))
- qkv_up_grad: float32 [128, 2304], P(None, ('img', 'tile'))
- proj_down_grad: float32 [768, 128], P(('img', 'tile'))
- proj_up_grad: float32 [128, 768], P(None, ('img', 'tile'))
- expand_down_grad: float32 [768, 128], P(('img', 'tile'))
- expand_up_grad: float32 [128, 3072], P(None, ('img', 'tile'))
- reduce_down_grad: float32 [3072, 128], P(('img', 'tile'))
- reduce_up_grad: float32 [128, 768], P(None, ('img', 'tile'))
The draws below stay inside these ranges and needn't reach their ends.
Inputs may be any that keep to these rules, and one draw needn't show every extreme that they name: `slot_mask`: slots 0 to 2 hold images and slot 23 is empty.
All inputs are finite; a program needn't handle non-finite values.
Results may differ from the reference program's by a relative error of at most 0.013.
Values may be sent and summed in bfloat16 or wider, within the bound.
A program may use at most 192 MiB of HBM per device.

```python
import math
import jax
import jax.numpy as jnp
from jax import lax

D = 768
HEADS = 24
FF = 3072
HEAD = 32
WIN = 12
SHIFT = 6
TILE_TOK = 144
RANK = 16
ADAPT = 8
SLOT_DEV = 3
SLOTS = 24


def draw_slot_mask(key, part):
    drawn_values = jax.random.randint(key, (SLOTS,), 0, 128)
    occupied = (drawn_values < 113).astype(jnp.int32)
    position = jnp.arange(SLOTS, dtype=jnp.int32)
    leading = jnp.where(position < SLOT_DEV, 1, occupied)
    return jnp.where(position == SLOTS - 1, 0, leading).astype(jnp.int32)


def with_ends(result, rng, low, top_value):
    longest = result.shape.index(max(result.shape))
    spots = []
    for shift in (0, 1):
        where = [jax.random.randint(jax.random.fold_in(rng, axis), (), 0, length) for axis, length in enumerate(result.shape)]
        where[longest] = (where[longest] + shift) % result.shape[longest]
        spots.append(tuple(where))
    return result.at[spots[0]].set(low).at[spots[1]].set(top_value)


def shard_levels(stream_key, dims, split, least, largest):
    loudness = 1.0
    for dim, blocks in split:
        steps = jax.random.uniform(jax.random.fold_in(jax.random.fold_in(stream_key, 6), dim), (blocks,), jnp.float32, least / len(split), largest / len(split))
        loudness = loudness * jnp.repeat(jnp.exp(steps), dims[dim] // blocks).reshape((-1,) + (1,) * (len(dims) - 1 - dim))
    return loudness


def gaussian(stream_key, shape, scale, bound, shards=(), kind=jnp.bfloat16):
    loudness = shard_levels(stream_key, shape, shards, -0.22, 0.18) if shards else 1.0
    result = jax.random.normal(stream_key, shape, jnp.float32) * scale * loudness
    return jnp.minimum(jnp.maximum(result, -bound), bound).astype(kind)


def setup_inputs(seed: int = 0) -> dict:
    key_of = jax.random.split(jax.random.key(seed), 26)
    return {
        "tokens": gaussian(key_of[0], (SLOTS, 4, TILE_TOK, D), 1.0, 6.0, ((0, 8), (1, 4))),
        "qkv_weight": gaussian(key_of[1], (D, 3 * D), D ** -0.5, 0.21875, ((0, 32),)),
        "proj_weight": gaussian(key_of[2], (D, D), (D // 16) ** -0.5, 0.875, ((0, 32),)),
        "expand_weight": gaussian(key_of[3], (D, FF), D ** -0.5, 0.21875, ((0, 32),)),
        "reduce_weight": gaussian(key_of[4], (FF, D), FF ** -0.5, 0.109375, ((0, 32),)),
        "qkv_down": gaussian(key_of[5], (D, ADAPT * RANK), D ** -0.5, 0.21875, ((0, 32),)),
        "qkv_up": gaussian(key_of[6], (ADAPT * RANK, 3 * D), RANK ** -0.5, 1.5, ((1, 32),)),
        "proj_down": gaussian(key_of[7], (D, ADAPT * RANK), D ** -0.5, 0.21875, ((0, 32),)),
        "proj_up": gaussian(key_of[8], (ADAPT * RANK, D), RANK ** -0.5, 1.5, ((1, 32),)),
        "expand_down": gaussian(key_of[9], (D, ADAPT * RANK), D ** -0.5, 0.21875, ((0, 32),)),
        "expand_up": gaussian(key_of[10], (ADAPT * RANK, FF), RANK ** -0.5, 1.5, ((1, 32),)),
        "reduce_down": gaussian(key_of[11], (FF, ADAPT * RANK), FF ** -0.5, 0.109375, ((0, 32),)),
        "reduce_up": gaussian(key_of[12], (ADAPT * RANK, D), RANK ** -0.5, 1.5, ((1, 32),)),
        "norm1_gain": jnp.clip(1.0 + 0.1 * jax.random.normal(key_of[13], (D,), jnp.float32), 0.5, 1.5),
        "norm1_bias": gaussian(key_of[14], (D,), 0.5, 3.0, (), jnp.float32),
        "norm2_gain": jnp.clip(1.0 + 0.1 * jax.random.normal(key_of[15], (D,), jnp.float32), 0.5, 1.5),
        "norm2_bias": gaussian(key_of[16], (D,), 0.5, 3.0, (), jnp.float32),
        "qkv_bias": gaussian(key_of[17], (3 * D,), 0.5, 3.0, (), jnp.float32),
        "proj_bias": gaussian(key_of[18], (D,), 0.5, 3.0, (), jnp.float32),
        "expand_bias": gaussian(key_of[19], (FF,), 0.5, 3.0, (), jnp.float32),
        "reduce_bias": gaussian(key_of[20], (D,), 0.5, 3.0, (), jnp.float32),
        "rel_table": gaussian(key_of[21], ((2 * WIN - 1) * (2 * WIN - 1), HEADS), 1.0, 4.0, (), jnp.float32),
        "slot_mask": draw_slot_mask(jax.random.fold_in(key_of[25], 71), 0),
        "adapter_index": with_ends(jax.random.randint(key_of[23], (SLOTS, 4), 0, ADAPT), jax.random.fold_in(key_of[23], 1), 0, ADAPT - 1).astype(jnp.int32),
        "cotangent": gaussian(key_of[24], (SLOTS, 4, TILE_TOK, D), 1.0, 6.0, ((0, 8), (1, 4))),
    }


@jax.custom_vjp
def low(v):
    return lax.optimization_barrier(v.astype(jnp.bfloat16)).astype(jnp.float32)

@jax.custom_vjp
def low_back(v):
    return v

def low_keep(v):
    return (low(v), None)

def low_pass(kept, grad):
    return (grad,)

def back_keep(v):
    return (v, None)

def back_low(kept, grad):
    return (low(grad),)
low.defvjp(low_keep, low_pass)
low_back.defvjp(back_keep, back_low)
norm_eps = 1e-05
lowrank_scale = 0.25
mask_fill = -100.0
maximal_precision = lax.Precision.HIGHEST

def regroup(values):
    group_size = values.shape[0]
    channels = values.shape[-1]
    image_plane = values.reshape(group_size, 2, 2, WIN, WIN, channels)
    return image_plane.transpose(0, 1, 3, 2, 4, 5).reshape(group_size, 2 * WIN, 2 * WIN, channels)

def split_quads(image_plane):
    group_size = image_plane.shape[0]
    channels = image_plane.shape[-1]
    blocks = image_plane.reshape(group_size, 2, WIN, 2, WIN, channels)
    return blocks.transpose(0, 1, 3, 2, 4, 5).reshape(group_size, 4, WIN * WIN, channels)

def to_windows(values):
    return split_quads(jnp.roll(regroup(values), (-SHIFT, -SHIFT), axis=(1, 2)))

def to_tiles(values):
    return split_quads(jnp.roll(regroup(values), (SHIFT, SHIFT), axis=(1, 2)))

def attention_bias(rel_table):
    coords = jnp.arange(WIN * WIN, dtype=jnp.int32)
    row_of = coords // WIN
    col_of = coords % WIN
    lookup = (row_of[:, None] - row_of[None, :] + WIN - 1) * (2 * WIN - 1) + col_of[:, None] - col_of[None, :] + WIN - 1
    relative = jnp.transpose(rel_table[lookup], (2, 0, 1))
    second_half = (jnp.arange(WIN, dtype=jnp.int32) >= WIN - SHIFT).astype(jnp.int32)
    mask_list = []
    for window in range(4):
        row_label = window // 2 * (1 + second_half)
        col_label = window % 2 * (1 + second_half)
        labels = (3 * row_label[:, None] + col_label[None, :]).reshape(-1)
        mask_list.append(jnp.where(labels[:, None] != labels[None, :], mask_fill, 0.0))
    region = jnp.stack(mask_list).astype(jnp.float32)
    return relative[None, :, :, :] + region[:, None, :, :]

def layer_norm(values, gain_vec, offset):
    center = values - lax.optimization_barrier(jnp.mean(values, axis=-1, keepdims=True))
    spread = lax.optimization_barrier(jnp.mean(center * center, axis=-1, keepdims=True))
    return center * lax.rsqrt(spread + norm_eps) * gain_vec + offset

def project(inputs, weight, bias_vec):
    return jnp.einsum('gwtc,co->gwto', inputs, weight, precision=maximal_precision) + bias_vec

def adapter(inputs, down_map, raise_matrix, column_mask):
    compressed_rows = jnp.einsum('gwtc,cr->gwtr', inputs, down_map, precision=maximal_precision) * column_mask[:, None, None, :]
    compressed_rows = low_back(low(compressed_rows))
    return lowrank_scale * jnp.einsum('qykl,lp->qykp', compressed_rows, raise_matrix, precision=maximal_precision)

def block_forward(tokens, adapters, frozen, columns, keep, bias_all):
    qkv_weight, proj_weight, expand_weight, reduce_weight, norm1_gain, norm1_bias, norm2_gain, norm2_bias, qkv_bias, proj_bias, expand_bias, reduce_bias = frozen
    qkv_down, qkv_up, proj_down, proj_up, expand_down, expand_up, reduce_down, reduce_up = adapters
    group_size = tokens.shape[0]
    head_scale = 1.0 / math.sqrt(HEAD)
    windows = to_windows(tokens)
    normed = low_back(low(layer_norm(windows, norm1_gain, norm1_bias)))
    packed = project(normed, qkv_weight, qkv_bias) + adapter(normed, qkv_down, qkv_up, columns[:, 0])
    packed = low_back(low(packed))
    head_view = packed.reshape(group_size, 4, WIN * WIN, 3, HEADS, HEAD)
    queries = head_view[:, :, :, 0]
    keys_all = head_view[:, :, :, 1]
    values_all = head_view[:, :, :, 2]
    scores = jnp.einsum('gwqhd,gwkhd->gwhqk', queries, keys_all, precision=maximal_precision) * head_scale + bias_all[None]
    scores = low_back(scores)
    row_max = lax.optimization_barrier(jnp.max(scores, axis=-1, keepdims=True))
    expons = jnp.exp(scores - row_max)
    attention = low(expons / lax.optimization_barrier(jnp.sum(expons, axis=-1, keepdims=True)))
    context = jnp.einsum('gwhqk,gwkhd->gwqhd', attention, values_all, precision=maximal_precision).reshape(group_size, 4, WIN * WIN, D)
    context = low_back(low(context))
    attended = project(context, proj_weight, proj_bias) + adapter(context, proj_down, proj_up, columns[:, 1])
    attended = low_back(attended)
    middle = windows + attended
    second = low(layer_norm(middle, norm2_gain, norm2_bias))
    expanded = project(second, expand_weight, expand_bias) + adapter(second, expand_down, expand_up, columns[:, 2])
    expanded = low_back(expanded)
    activated = low(0.5 * expanded * (1.0 + jax.scipy.special.erf(expanded / math.sqrt(2.0))))
    branch = project(activated, reduce_weight, reduce_bias) + adapter(activated, reduce_down, reduce_up, columns[:, 3])
    branch = low_back(branch)
    return to_tiles((middle + branch) * keep[:, None, None, None])

def add_up(first_sum, second_sum):
    return first_sum + second_sum

def reference(tokens, qkv_weight, proj_weight, expand_weight, reduce_weight, qkv_down, qkv_up, proj_down, proj_up, expand_down, expand_up, reduce_down, reduce_up, norm1_gain, norm1_bias, norm2_gain, norm2_bias, qkv_bias, proj_bias, expand_bias, reduce_bias, rel_table, slot_mask, adapter_index, cotangent):
    frozen = tuple((array_in.astype(jnp.float32) for array_in in (qkv_weight, proj_weight, expand_weight, reduce_weight, norm1_gain, norm1_bias, norm2_gain, norm2_bias, qkv_bias, proj_bias, expand_bias, reduce_bias)))
    adapters = tuple((array_in.astype(jnp.float32) for array_in in (qkv_down, qkv_up, proj_down, proj_up, expand_down, expand_up, reduce_down, reduce_up)))
    selected = (adapter_index[:, :, None] == jnp.arange(ADAPT, dtype=jnp.int32)[None, None, :]).astype(jnp.float32)
    columns = jnp.repeat(selected, RANK, axis=2)
    keep = slot_mask.astype(jnp.float32)
    bias_all = attention_bias(rel_table.astype(jnp.float32))
    groups = SLOTS // 4

    def shaped(values):
        return values.reshape((groups, 4) + values.shape[1:])

    def one_group(totals, pieces):
        group_tokens, group_cot, group_cols, group_keep = pieces

        def forward(token_values, adapter_values):
            return block_forward(token_values, adapter_values, frozen, group_cols, group_keep, bias_all)
        outputs, pullback = jax.vjp(forward, group_tokens.astype(jnp.float32), adapters)
        grad_tokens, grad_adapters = pullback(group_cot.astype(jnp.float32))
        totals = jax.tree.map(add_up, totals, grad_adapters)
        return (totals, (outputs.astype(jnp.bfloat16), grad_tokens.astype(jnp.bfloat16)))
    initial = tuple((jnp.zeros(array_in.shape, jnp.float32) for array_in in adapters))
    totals, (outputs, back_grads) = lax.scan(one_group, initial, (shaped(tokens), shaped(cotangent), shaped(columns), shaped(keep)))
    block_output = outputs.reshape(tokens.shape)
    input_grad = back_grads.reshape(tokens.shape)
    return (block_output, input_grad, totals[0], totals[1], totals[2], totals[3], totals[4], totals[5], totals[6], totals[7])
```

```python
import math

import jax
import jax.numpy as jnp
from jax import lax
from jax.sharding import PartitionSpec as P

HEADS = 24
WIN = 12
SHIFT = 6
RANK = 16
ADAPT = 8
LANES = 128


norm_eps = 1e-05
lowrank_scale = 0.25
mask_fill = -100.0
maximal_precision = lax.Precision.HIGHEST
both_axes = ("img", "tile")


def full_matrix(matrix_one, matrix_two):
    return jnp.dot(matrix_one, matrix_two, preferred_element_type=jnp.float32)


def full_left_factor(matrix_one, matrix_two):
    return lax.dot_general(
        matrix_one, matrix_two, (((0,), (0,)), ((), ())), preferred_element_type=jnp.float32
    )


def full_right_factor(matrix_one, matrix_two):
    return lax.dot_general(
        matrix_one, matrix_two, (((1,), (1,)), ((), ())), preferred_element_type=jnp.float32
    )


def exchange_tables(slot_count, row_half, col_half):
    quarter = SHIFT * SHIFT
    padded = -(-slot_count * quarter // 16) * 16
    place = jnp.arange(4 * padded)
    dest, rest = place // padded, place % padded
    slot, spot = rest // quarter, rest % quarter
    row_part = jnp.where(dest // 2 == row_half, 1, 0)
    col_part = jnp.where(dest % 2 == col_half, 1, 0)
    tile_row = (
        slot * WIN * WIN
        + (SHIFT * row_part + spot // SHIFT) * WIN
        + SHIFT * col_part
        + spot % SHIFT
    )
    tile_row = jnp.where(rest < slot_count * quarter, tile_row, -1)
    token = jnp.arange(slot_count * WIN * WIN)
    slot, spot = token // (WIN * WIN), token % (WIN * WIN)
    row_at, col_at = spot // WIN, spot % WIN
    source_row = jnp.where(row_at < SHIFT, row_half, 1 - row_half)
    source_col = jnp.where(col_at < SHIFT, col_half, 1 - col_half)
    arrived_row = (
        (2 * source_row + source_col) * padded
        + slot * quarter
        + (row_at % SHIFT) * SHIFT
        + col_at % SHIFT
    )
    rows_all = slot_count * WIN * WIN
    send_pick = (tile_row[:, None] == jnp.arange(rows_all)[None, :]).astype(jnp.bfloat16)
    window_pick = (arrived_row[:, None] == place[None, :]).astype(jnp.bfloat16)
    return send_pick, window_pick


def swap_quarters(rows_low):
    blocks = rows_low.reshape(4, rows_low.shape[0] // 4, rows_low.shape[1])
    arrived = lax.all_to_all(blocks, "tile", split_axis=0, concat_axis=0, tiled=True)
    return arrived.reshape(rows_low.shape)


def window_bias(rel_table, row_half, col_half):
    extent = 2 * WIN - 1
    offsets = jnp.arange(WIN)[:, None] - jnp.arange(WIN)[None, :] + WIN - 1
    picker = (offsets[:, :, None] == jnp.arange(extent)[None, None, :]).astype(jnp.float32)
    rel_grid = rel_table.reshape(extent, extent, HEADS)
    partial_sum = jnp.einsum("jlq,pqh->pjlh", picker, rel_grid, precision=maximal_precision)
    relative = jnp.einsum(
        "ikp,pjlh->hijkl", picker, partial_sum, precision=maximal_precision
    ).reshape(HEADS, WIN * WIN, WIN * WIN)
    second_half = (jnp.arange(WIN) >= WIN - SHIFT).astype(jnp.int32)
    row_label = row_half * (1 + second_half)
    col_label = col_half * (1 + second_half)
    labels = (3 * row_label[:, None] + col_label[None, :]).reshape(-1)
    region = jnp.where(labels[:, None] != labels[None, :], mask_fill, 0.0).astype(jnp.float32)
    return relative + region[None]


def norm_forward(values, gain_vec, offset):
    center = values - jnp.mean(values, axis=-1, keepdims=True)
    scaled = lax.rsqrt(jnp.mean(center * center, axis=-1, keepdims=True) + norm_eps)
    normal = center * scaled
    return (normal * gain_vec + offset, normal, scaled)


def norm_backward(grad_out, gain_vec, normal, scaled):
    grad_normal = grad_out * gain_vec
    return scaled * (
        grad_normal
        - jnp.mean(grad_normal, axis=-1, keepdims=True)
        - normal * jnp.mean(grad_normal * normal, axis=-1, keepdims=True)
    )


def gelu_value(values):
    return 0.5 * values * (1.0 + jax.scipy.special.erf(values / math.sqrt(2.0)))


def gelu_slope(values):
    return 0.5 * (1.0 + jax.scipy.special.erf(values / math.sqrt(2.0))) + values * jnp.exp(
        -0.5 * values * values
    ) / math.sqrt(2.0 * math.pi)


def adapter_forward(inputs, down_map, raise_turned, row_columns):
    compressed_rows = (full_matrix(inputs, down_map) * row_columns).astype(jnp.bfloat16)
    return (lowrank_scale * full_right_factor(compressed_rows, raise_turned), compressed_rows)


def adapter_backward(
    inputs, compressed_rows, gradient_rank_space, down_map, raise_turned, row_columns
):
    gradient_raise_turned = lowrank_scale * full_left_factor(gradient_rank_space, compressed_rows)
    gradient_compressed = (lowrank_scale * full_matrix(gradient_rank_space, raise_turned)).astype(
        jnp.bfloat16
    ) * row_columns.astype(jnp.bfloat16)
    grad_down = full_left_factor(inputs, gradient_compressed)
    return (grad_down, gradient_raise_turned, full_right_factor(gradient_compressed, down_map))


def split_heads(packed_low, slot_count):
    head_view = packed_low.reshape(slot_count, -1, 3, HEADS, packed_low.shape[1] // (3 * HEADS))
    return (head_view[:, :, 0], head_view[:, :, 1], head_view[:, :, 2])


def attention_scores(queries, keys_all, bias_all, head_scale):
    return (
        jnp.einsum("sqhd,skhd->shqk", queries, keys_all, preferred_element_type=jnp.float32)
        * head_scale
        + bias_all[None]
    )


def attention_forward(packed_low, bias_all, slot_count, head_scale):
    queries, keys_all, values_all = split_heads(packed_low, slot_count)
    scores = attention_scores(queries, keys_all, bias_all, head_scale)
    row_max = jnp.max(scores, axis=-1, keepdims=True)
    expons = jnp.exp(scores - row_max)
    totals = jnp.sum(expons, axis=-1, keepdims=True)
    attention_low = (expons / totals).astype(jnp.bfloat16)
    log_total = row_max + jnp.log(totals)
    context = jnp.einsum(
        "shqk,skhd->sqhd", attention_low, values_all, preferred_element_type=jnp.float32
    )
    return (context.reshape(packed_low.shape[0], -1).astype(jnp.bfloat16), log_total)


def attention_backward(packed_low, bias_all, log_total, grad_context, slot_count, head_scale):
    queries, keys_all, values_all = split_heads(packed_low, slot_count)
    scores = attention_scores(queries, keys_all, bias_all, head_scale)
    attention = jnp.exp(scores - log_total)
    attention_low = attention.astype(jnp.bfloat16)
    grad_heads = grad_context.reshape(queries.shape)
    grad_values = jnp.einsum(
        "shqk,sqhd->skhd", attention_low, grad_heads, preferred_element_type=jnp.float32
    )
    grad_weights = jnp.einsum(
        "sqhd,skhd->shqk", grad_heads, values_all, preferred_element_type=jnp.float32
    )
    grad_scores = (
        attention * (grad_weights - jnp.sum(attention * grad_weights, axis=-1, keepdims=True))
    ).astype(jnp.bfloat16)
    grad_queries = (
        jnp.einsum("shqk,skhd->sqhd", grad_scores, keys_all, preferred_element_type=jnp.float32)
        * head_scale
    )
    grad_keys = (
        jnp.einsum("shqk,sqhd->skhd", grad_scores, queries, preferred_element_type=jnp.float32)
        * head_scale
    )
    stacked = jnp.stack([grad_queries, grad_keys, grad_values], axis=2)
    return stacked.reshape(packed_low.shape).astype(jnp.bfloat16)


def to_panels(matrix):
    rows = matrix.shape[0]
    return matrix.reshape(rows, -1, LANES).transpose(1, 0, 2).reshape(-1, LANES)


def gather_all(by_rows, by_columns):
    pieces = [to_panels(matrix) for matrix in by_rows] + [matrix.T for matrix in by_columns]
    packed = jnp.concatenate(pieces, axis=0)
    everything = lax.all_gather(packed, both_axes, axis=0, tiled=False)
    devices = everything.shape[0]
    whole, start = [], 0
    for matrix in by_rows:
        rows, columns = matrix.shape
        size = rows * columns // LANES
        part = everything[:, start : start + size].reshape(devices, columns // LANES, rows, LANES)
        whole.append(part.transpose(0, 2, 1, 3).reshape(devices * rows, columns))
        start += size
    for matrix in by_columns:
        size = matrix.shape[1]
        whole.append(everything[:, start : start + size].reshape(devices * size, LANES))
        start += size
    return whole


def scatter_sums(gradients, devices):
    pieces = [grad.reshape(devices, -1, LANES) for grad in gradients]
    packed = jnp.concatenate(pieces, axis=1)
    mine = lax.psum_scatter(packed, both_axes, scatter_dimension=0, tiled=False)
    own, start = [], 0
    for piece in pieces:
        own.append(mine[start : start + piece.shape[1]])
        start += piece.shape[1]
    return own


def shards(
    devices,
    tokens,
    qkv_weight,
    proj_weight,
    expand_weight,
    reduce_weight,
    qkv_down,
    qkv_up,
    proj_down,
    proj_up,
    expand_down,
    expand_up,
    reduce_down,
    reduce_up,
    norm1_gain,
    norm1_bias,
    norm2_gain,
    norm2_bias,
    qkv_bias,
    proj_bias,
    expand_bias,
    reduce_bias,
    rel_table,
    slot_mask,
    adapter_index,
    cotangent,
):
    slot_count = tokens.shape[0]
    tile_tokens = tokens.shape[2]
    model_width = tokens.shape[3]
    rows_all = slot_count * tile_tokens
    tile_place = lax.axis_index("tile")
    row_half = tile_place // 2
    col_half = tile_place % 2
    head_scale = 1.0 / math.sqrt(model_width // HEADS)
    (
        qkv_full,
        proj_full,
        expand_full,
        reduce_full,
        qkv_d,
        proj_d,
        expand_d,
        reduce_d,
        qkv_u,
        proj_u,
        expand_u,
        reduce_u,
    ) = gather_all(
        (
            qkv_weight,
            proj_weight,
            expand_weight,
            reduce_weight,
            qkv_down,
            proj_down,
            expand_down,
            reduce_down,
        ),
        (qkv_up, proj_up, expand_up, reduce_up),
    )
    selected = (
        adapter_index[:, :, None] == jnp.arange(ADAPT, dtype=jnp.int32)[None, None, :]
    ).astype(jnp.float32)
    columns = jnp.repeat(jnp.repeat(selected, RANK, axis=2), tile_tokens, axis=0)
    keep_rows = jnp.repeat(slot_mask.astype(jnp.float32), tile_tokens)[:, None]
    bias_all = window_bias(rel_table, row_half, col_half)
    send_pick, window_pick = exchange_tables(slot_count, row_half, col_half)
    both = jnp.concatenate(
        [tokens.reshape(rows_all, model_width), cotangent.reshape(rows_all, model_width)], axis=1
    )
    arrived = swap_quarters(full_matrix(send_pick, both).astype(jnp.bfloat16))
    both = full_matrix(window_pick, arrived)
    inputs = both[:, :model_width]
    grad_rows = both[:, model_width:] * keep_rows

    first_normed, first_normal, first_scaled = norm_forward(inputs, norm1_gain, norm1_bias)
    window_in = first_normed.astype(jnp.bfloat16)
    qkv_term, qkv_reduced = adapter_forward(window_in, qkv_d, qkv_u, columns[:, 0])
    packed_low = (full_matrix(window_in, qkv_full) + qkv_bias + qkv_term).astype(jnp.bfloat16)
    context_low, log_total = attention_forward(packed_low, bias_all, slot_count, head_scale)
    proj_term, proj_reduced = adapter_forward(context_low, proj_d, proj_u, columns[:, 1])
    attended = full_matrix(context_low, proj_full) + proj_bias + proj_term
    middle = inputs + attended
    second_normed, second_normal, second_scaled = norm_forward(middle, norm2_gain, norm2_bias)
    second_low = second_normed.astype(jnp.bfloat16)
    expand_term, expand_reduced = adapter_forward(second_low, expand_d, expand_u, columns[:, 2])
    expanded = full_matrix(second_low, expand_full) + expand_bias + expand_term
    activated = gelu_value(expanded).astype(jnp.bfloat16)
    reduce_term, reduce_reduced = adapter_forward(activated, reduce_d, reduce_u, columns[:, 3])
    branch = full_matrix(activated, reduce_full) + reduce_bias + reduce_term
    block_windows = ((middle + branch) * keep_rows).astype(jnp.bfloat16)

    grad_branch = grad_rows.astype(jnp.bfloat16)
    reduce_dgrad, reduce_ugrad, extra_term = adapter_backward(
        activated, reduce_reduced, grad_branch, reduce_d, reduce_u, columns[:, 3]
    )
    grad_activated = full_right_factor(grad_branch, reduce_full) + extra_term
    grad_expanded = (grad_activated * gelu_slope(expanded)).astype(jnp.bfloat16)
    expand_dgrad, expand_ugrad, extra_term = adapter_backward(
        second_low, expand_reduced, grad_expanded, expand_d, expand_u, columns[:, 2]
    )
    grad_second = full_right_factor(grad_expanded, expand_full) + extra_term
    grad_middle = grad_rows + norm_backward(grad_second, norm2_gain, second_normal, second_scaled)
    grad_attended = grad_middle.astype(jnp.bfloat16)
    proj_dgrad, proj_ugrad, extra_term = adapter_backward(
        context_low, proj_reduced, grad_attended, proj_d, proj_u, columns[:, 1]
    )
    grad_context = (full_right_factor(grad_attended, proj_full) + extra_term).astype(jnp.bfloat16)
    grad_packed = attention_backward(
        packed_low, bias_all, log_total, grad_context, slot_count, head_scale
    )
    qkv_dgrad, qkv_ugrad, extra_term = adapter_backward(
        window_in, qkv_reduced, grad_packed, qkv_d, qkv_u, columns[:, 0]
    )
    grad_normed = (full_right_factor(grad_packed, qkv_full) + extra_term).astype(jnp.bfloat16)
    grad_inputs = grad_middle + norm_backward(
        grad_normed.astype(jnp.float32), norm1_gain, first_normal, first_scaled
    )
    grad_windows = grad_inputs.astype(jnp.bfloat16)

    both = jnp.concatenate([block_windows, grad_windows], axis=1)
    arrived = swap_quarters(full_left_factor(window_pick, both).astype(jnp.bfloat16))
    both = full_left_factor(send_pick, arrived).astype(jnp.bfloat16)
    summed = scatter_sums(
        (
            qkv_dgrad,
            proj_dgrad,
            expand_dgrad,
            reduce_dgrad,
            qkv_ugrad,
            proj_ugrad,
            expand_ugrad,
            reduce_ugrad,
        ),
        devices,
    )
    return (
        both[:, :model_width].reshape(tokens.shape),
        both[:, model_width:].reshape(tokens.shape),
        summed[0],
        summed[4].T,
        summed[1],
        summed[5].T,
        summed[2],
        summed[6].T,
        summed[3],
        summed[7].T,
    )


def solution(mesh):
    rows = P(both_axes, None)
    columns = P(None, both_axes)
    image = P("img", "tile", None, None)
    placed = (
        (image,)
        + (rows,) * 4
        + (rows, columns) * 4
        + (P(),) * 9
        + (P("img"), P("img", None), image)
    )

    def step(*arrays):
        return shards(mesh.size, *arrays)

    return jax.shard_map(
        step,
        mesh=mesh,
        in_specs=placed,
        out_specs=(image, image) + (rows, columns) * 4,
        check_vma=False,
    )
```

```python
import functools
import math

import jax
import jax.numpy as jnp
from jax import lax
from jax.experimental import pallas as pl
from jax.experimental.pallas import tpu as pltpu
from jax.sharding import PartitionSpec as P

HEADS = 24
WIN = 12
SHIFT = 6
RANK = 16
ADAPT = 8
LANES = 128
HEAD = 32
GROUP = LANES // HEAD


norm_eps = 1e-05
lowrank_scale = 0.25
mask_fill = -100.0
head_scale = 1.0 / math.sqrt(HEAD)
maximal_precision = lax.Precision.HIGHEST
both_axes = ("img", "tile")


def full_matrix(matrix_one, matrix_two):
    return jnp.dot(matrix_one, matrix_two, preferred_element_type=jnp.float32)


def full_left_factor(matrix_one, matrix_two):
    return lax.dot_general(
        matrix_one, matrix_two, (((0,), (0,)), ((), ())), preferred_element_type=jnp.float32
    )


def full_right_factor(matrix_one, matrix_two):
    return lax.dot_general(
        matrix_one, matrix_two, (((1,), (1,)), ((), ())), preferred_element_type=jnp.float32
    )


def exchange_tables(slot_count, row_half, col_half):
    quarter = SHIFT * SHIFT
    padded = -(-slot_count * quarter // 16) * 16
    place = jnp.arange(4 * padded)
    dest, rest = place // padded, place % padded
    slot, spot = rest // quarter, rest % quarter
    row_part = jnp.where(dest // 2 == row_half, 1, 0)
    col_part = jnp.where(dest % 2 == col_half, 1, 0)
    tile_row = (
        slot * WIN * WIN
        + (SHIFT * row_part + spot // SHIFT) * WIN
        + SHIFT * col_part
        + spot % SHIFT
    )
    tile_row = jnp.where(rest < slot_count * quarter, tile_row, -1)
    token = jnp.arange(slot_count * WIN * WIN)
    slot, spot = token // (WIN * WIN), token % (WIN * WIN)
    row_at, col_at = spot // WIN, spot % WIN
    source_row = jnp.where(row_at < SHIFT, row_half, 1 - row_half)
    source_col = jnp.where(col_at < SHIFT, col_half, 1 - col_half)
    arrived_row = (
        (2 * source_row + source_col) * padded
        + slot * quarter
        + (row_at % SHIFT) * SHIFT
        + col_at % SHIFT
    )
    rows_all = slot_count * WIN * WIN
    send_pick = (tile_row[:, None] == jnp.arange(rows_all)[None, :]).astype(jnp.bfloat16)
    window_pick = (arrived_row[:, None] == place[None, :]).astype(jnp.bfloat16)
    return send_pick, window_pick


def swap_quarters(rows_low):
    blocks = rows_low.reshape(4, rows_low.shape[0] // 4, rows_low.shape[1])
    arrived = lax.all_to_all(blocks, "tile", split_axis=0, concat_axis=0, tiled=True)
    return arrived.reshape(rows_low.shape)


def norm_forward(values, gain_vec, offset):
    center = values - jnp.mean(values, axis=-1, keepdims=True)
    scaled = lax.rsqrt(jnp.mean(center * center, axis=-1, keepdims=True) + norm_eps)
    normal = center * scaled
    return (normal * gain_vec + offset, normal, scaled)


def norm_backward(grad_out, gain_vec, normal, scaled):
    grad_normal = grad_out * gain_vec
    return scaled * (
        grad_normal
        - jnp.mean(grad_normal, axis=-1, keepdims=True)
        - normal * jnp.mean(grad_normal * normal, axis=-1, keepdims=True)
    )


def gelu_value(values):
    return 0.5 * values * (1.0 + jax.scipy.special.erf(values / math.sqrt(2.0)))


def gelu_slope(values):
    return 0.5 * (1.0 + jax.scipy.special.erf(values / math.sqrt(2.0))) + values * jnp.exp(
        -0.5 * values * values
    ) / math.sqrt(2.0 * math.pi)


def adapter_forward(inputs, down_map, raise_turned, row_columns):
    compressed_rows = (full_matrix(inputs, down_map) * row_columns).astype(jnp.bfloat16)
    return (lowrank_scale * full_right_factor(compressed_rows, raise_turned), compressed_rows)


def adapter_backward(
    inputs, compressed_rows, gradient_rank_space, down_map, raise_turned, row_columns
):
    gradient_raise_turned = lowrank_scale * full_left_factor(gradient_rank_space, compressed_rows)
    gradient_compressed = (lowrank_scale * full_matrix(gradient_rank_space, raise_turned)).astype(
        jnp.bfloat16
    ) * row_columns.astype(jnp.bfloat16)
    grad_down = full_left_factor(inputs, gradient_compressed)
    return (grad_down, gradient_raise_turned, full_right_factor(gradient_compressed, down_map))


def head_lanes(group):
    lane = lax.broadcasted_iota(jnp.int32, (1, LANES), 1)
    return lane // HEAD == group


def stack_heads(values):
    zero = jnp.zeros_like(values)
    return jnp.concatenate(
        [jnp.where(head_lanes(group), values, zero) for group in range(GROUP)], axis=0
    )


def merge_heads(stacked):
    tall = stacked.shape[0] // GROUP
    merged = jnp.where(head_lanes(0), stacked[:tall], 0.0)
    for group in range(1, GROUP):
        merged = merged + jnp.where(
            head_lanes(group), stacked[group * tall : (group + 1) * tall], 0.0
        )
    return merged


def softmax_stacked(query_stack, keys, bias):
    scores = full_right_factor(query_stack, keys) * head_scale + bias
    expons = jnp.exp(scores - jnp.max(scores, axis=-1, keepdims=True))
    return expons * (1.0 / jnp.sum(expons, axis=-1, keepdims=True))


def attention_forward_kernel(slot_count, query_ref, key_ref, value_ref, bias_ref, context_ref):
    tall = WIN * WIN
    bias = bias_ref[...].reshape(GROUP * tall, tall)
    for slot in range(slot_count):
        here = slice(slot * tall, (slot + 1) * tall)
        weights = softmax_stacked(stack_heads(query_ref[here, :]), key_ref[here, :], bias)
        context = full_matrix(weights.astype(jnp.bfloat16), value_ref[here, :])
        context_ref[here, :] = merge_heads(context).astype(jnp.bfloat16)


def attention_backward_kernel(
    slot_count, query_ref, key_ref, value_ref, grad_ref, bias_ref, packed_ref
):
    tall = WIN * WIN
    width = packed_ref.shape[1] // 3
    start = pl.multiple_of(pl.program_id(0) * LANES, LANES)
    bias = bias_ref[...].reshape(GROUP * tall, tall)
    for slot in range(slot_count):
        here = slice(slot * tall, (slot + 1) * tall)
        keys, values = key_ref[here, :], value_ref[here, :]
        query_stack = stack_heads(query_ref[here, :])
        grad_stack = stack_heads(grad_ref[here, :])
        weights = softmax_stacked(query_stack, keys, bias)
        grad_values = full_left_factor(weights.astype(jnp.bfloat16), grad_stack)
        grad_weights = full_right_factor(grad_stack, values)
        weighted = weights * grad_weights
        grad_scores = (
            weighted - weights * jnp.sum(weighted, axis=-1, keepdims=True)
        ).astype(jnp.bfloat16)
        grad_queries = merge_heads(full_matrix(grad_scores, keys)) * head_scale
        grad_keys = full_left_factor(grad_scores, query_stack) * head_scale
        for part, grad in enumerate((grad_queries, grad_keys, grad_values)):
            packed_ref[here, pl.ds(start + part * width, LANES)] = grad.astype(jnp.bfloat16)


def bias_kernel(strips_ref, place_ref, region_ref, bias_ref):
    strip = strips_ref[0]
    tall = WIN * WIN
    rows = []
    for row in range(WIN):
        offset = (WIN - 1 - row) * WIN
        rows.append(strip[:, offset : offset + tall])
    stacked = jnp.concatenate(rows, axis=0)
    upper = stacked.astype(jnp.bfloat16)
    rest = stacked - upper.astype(jnp.float32)
    middle = rest.astype(jnp.bfloat16)
    lower = (rest - middle.astype(jnp.float32)).astype(jnp.bfloat16)
    place = place_ref[...]
    picked = full_matrix(place, upper) + (full_matrix(place, middle) + full_matrix(place, lower))
    bias_ref[0] = picked + region_ref[...]


def window_bias(rel_table, row_half, col_half):
    extent = 2 * WIN - 1
    tall = WIN * WIN
    padded, long = 16, 3 * LANES
    spot = jnp.arange(padded * long)
    across, lane = spot // long, spot % long
    down, other = lane // WIN, lane % WIN
    wanted = (extent - 1 - down) * extent + across - other + WIN - 1
    wanted = jnp.where((across < WIN) & (down < extent), wanted, -1)
    picker = (jnp.arange(extent * extent)[:, None] == wanted[None, :]).astype(jnp.float32)
    strips = lax.dot_general(
        rel_table, picker, (((0,), (0,)), ((), ())), precision=maximal_precision
    ).reshape(HEADS, padded, long)
    token = jnp.arange(tall)
    place = (token // WIN * padded + token % WIN)[:, None] == jnp.arange(WIN * padded)[None, :]
    second_half = (jnp.arange(WIN) >= WIN - SHIFT).astype(jnp.int32)
    row_label = row_half * (1 + second_half)
    col_label = col_half * (1 + second_half)
    labels = (3 * row_label[:, None] + col_label[None, :]).reshape(-1)
    region = jnp.where(labels[:, None] != labels[None, :], mask_fill, 0.0).astype(jnp.float32)
    return pl.pallas_call(
        bias_kernel,
        grid=(HEADS,),
        in_specs=[
            pl.BlockSpec((1, padded, long), lambda head: (head, 0, 0)),
            pl.BlockSpec((tall, WIN * padded), lambda head: (0, 0)),
            pl.BlockSpec((tall, tall), lambda head: (0, 0)),
        ],
        out_specs=pl.BlockSpec((1, tall, tall), lambda head: (head, 0, 0)),
        out_shape=jax.ShapeDtypeStruct((HEADS, tall, tall), jnp.float32),
        name="bias_table",
    )(strips, place.astype(jnp.bfloat16), region)


def head_block(rows, first):
    return pl.BlockSpec((rows, LANES), lambda group: (0, first + group))


def attention_forward(packed_low, bias_all, slot_count):
    rows, width = packed_low.shape[0], packed_low.shape[1] // 3
    groups = width // LANES
    tall = WIN * WIN
    return pl.pallas_call(
        functools.partial(attention_forward_kernel, slot_count),
        grid=(groups,),
        in_specs=[head_block(rows, part * groups) for part in range(3)]
        + [pl.BlockSpec((GROUP, tall, tall), lambda group: (group, 0, 0))],
        out_specs=head_block(rows, 0),
        out_shape=jax.ShapeDtypeStruct((rows, width), jnp.bfloat16),
        name="attention_forward",
    )(packed_low, packed_low, packed_low, bias_all)


def attention_backward(packed_low, bias_all, grad_context, slot_count):
    rows, width = packed_low.shape[0], packed_low.shape[1] // 3
    groups = width // LANES
    tall = WIN * WIN
    return pl.pallas_call(
        functools.partial(attention_backward_kernel, slot_count),
        grid=(groups,),
        in_specs=[head_block(rows, part * groups) for part in range(3)]
        + [head_block(rows, 0), pl.BlockSpec((GROUP, tall, tall), lambda group: (group, 0, 0))],
        out_specs=pl.BlockSpec((rows, 3 * width), lambda group: (0, 0)),
        out_shape=jax.ShapeDtypeStruct((rows, 3 * width), jnp.bfloat16),
        name="attention_backward",
    )(packed_low, packed_low, packed_low, grad_context, bias_all)


def to_panels(matrix):
    rows = matrix.shape[0]
    return matrix.reshape(rows, -1, LANES).transpose(1, 0, 2).reshape(-1, LANES)


def gather_all(by_rows, by_columns):
    pieces = [to_panels(matrix) for matrix in by_rows] + [matrix.T for matrix in by_columns]
    packed = jnp.concatenate(pieces, axis=0)
    everything = lax.all_gather(packed, both_axes, axis=0, tiled=False)
    devices = everything.shape[0]
    whole, start = [], 0
    for matrix in by_rows:
        rows, columns = matrix.shape
        size = rows * columns // LANES
        part = everything[:, start : start + size].reshape(devices, columns // LANES, rows, LANES)
        whole.append(part.transpose(0, 2, 1, 3).reshape(devices * rows, columns))
        start += size
    for matrix in by_columns:
        size = matrix.shape[1]
        whole.append(everything[:, start : start + size].reshape(devices * size, LANES))
        start += size
    return whole


def scatter_sums(gradients, devices):
    pieces = [grad.reshape(devices, -1, LANES) for grad in gradients]
    packed = jnp.concatenate(pieces, axis=1)
    mine = lax.psum_scatter(packed, both_axes, scatter_dimension=0, tiled=False)
    own, start = [], 0
    for piece in pieces:
        own.append(mine[start : start + piece.shape[1]])
        start += piece.shape[1]
    return own


def shards(
    devices,
    tokens,
    qkv_weight,
    proj_weight,
    expand_weight,
    reduce_weight,
    qkv_down,
    qkv_up,
    proj_down,
    proj_up,
    expand_down,
    expand_up,
    reduce_down,
    reduce_up,
    norm1_gain,
    norm1_bias,
    norm2_gain,
    norm2_bias,
    qkv_bias,
    proj_bias,
    expand_bias,
    reduce_bias,
    rel_table,
    slot_mask,
    adapter_index,
    cotangent,
):
    slot_count = tokens.shape[0]
    tile_tokens = tokens.shape[2]
    model_width = tokens.shape[3]
    rows_all = slot_count * tile_tokens
    tile_place = lax.axis_index("tile")
    row_half = tile_place // 2
    col_half = tile_place % 2
    (
        qkv_full,
        proj_full,
        expand_full,
        reduce_full,
        qkv_d,
        proj_d,
        expand_d,
        reduce_d,
        qkv_u,
        proj_u,
        expand_u,
        reduce_u,
    ) = gather_all(
        (
            qkv_weight,
            proj_weight,
            expand_weight,
            reduce_weight,
            qkv_down,
            proj_down,
            expand_down,
            reduce_down,
        ),
        (qkv_up, proj_up, expand_up, reduce_up),
    )
    selected = (
        adapter_index[:, :, None] == jnp.arange(ADAPT, dtype=jnp.int32)[None, None, :]
    ).astype(jnp.float32)
    columns = jnp.repeat(jnp.repeat(selected, RANK, axis=2), tile_tokens, axis=0)
    keep_rows = jnp.repeat(slot_mask.astype(jnp.float32), tile_tokens)[:, None]
    bias_all = window_bias(rel_table, row_half, col_half)
    send_pick, window_pick = exchange_tables(slot_count, row_half, col_half)
    both = jnp.concatenate(
        [tokens.reshape(rows_all, model_width), cotangent.reshape(rows_all, model_width)], axis=1
    )
    arrived = swap_quarters(full_matrix(send_pick, both).astype(jnp.bfloat16))
    both = full_matrix(window_pick, arrived)
    inputs = both[:, :model_width]
    grad_rows = both[:, model_width:] * keep_rows

    first_normed, first_normal, first_scaled = norm_forward(inputs, norm1_gain, norm1_bias)
    window_in = first_normed.astype(jnp.bfloat16)
    qkv_term, qkv_reduced = adapter_forward(window_in, qkv_d, qkv_u, columns[:, 0])
    packed_low = (full_matrix(window_in, qkv_full) + qkv_bias + qkv_term).astype(jnp.bfloat16)
    context_low = attention_forward(packed_low, bias_all, slot_count)
    proj_term, proj_reduced = adapter_forward(context_low, proj_d, proj_u, columns[:, 1])
    attended = full_matrix(context_low, proj_full) + proj_bias + proj_term
    middle = inputs + attended
    second_normed, second_normal, second_scaled = norm_forward(middle, norm2_gain, norm2_bias)
    second_low = second_normed.astype(jnp.bfloat16)
    expand_term, expand_reduced = adapter_forward(second_low, expand_d, expand_u, columns[:, 2])
    expanded = full_matrix(second_low, expand_full) + expand_bias + expand_term
    activated = gelu_value(expanded).astype(jnp.bfloat16)
    reduce_term, reduce_reduced = adapter_forward(activated, reduce_d, reduce_u, columns[:, 3])
    branch = full_matrix(activated, reduce_full) + reduce_bias + reduce_term
    block_windows = ((middle + branch) * keep_rows).astype(jnp.bfloat16)

    grad_branch = grad_rows.astype(jnp.bfloat16)
    reduce_dgrad, reduce_ugrad, extra_term = adapter_backward(
        activated, reduce_reduced, grad_branch, reduce_d, reduce_u, columns[:, 3]
    )
    grad_activated = full_right_factor(grad_branch, reduce_full) + extra_term
    grad_expanded = (grad_activated * gelu_slope(expanded)).astype(jnp.bfloat16)
    expand_dgrad, expand_ugrad, extra_term = adapter_backward(
        second_low, expand_reduced, grad_expanded, expand_d, expand_u, columns[:, 2]
    )
    grad_second = full_right_factor(grad_expanded, expand_full) + extra_term
    grad_middle = grad_rows + norm_backward(grad_second, norm2_gain, second_normal, second_scaled)
    grad_attended = grad_middle.astype(jnp.bfloat16)
    proj_dgrad, proj_ugrad, extra_term = adapter_backward(
        context_low, proj_reduced, grad_attended, proj_d, proj_u, columns[:, 1]
    )
    grad_context = (full_right_factor(grad_attended, proj_full) + extra_term).astype(jnp.bfloat16)
    grad_packed = attention_backward(packed_low, bias_all, grad_context, slot_count)
    qkv_dgrad, qkv_ugrad, extra_term = adapter_backward(
        window_in, qkv_reduced, grad_packed, qkv_d, qkv_u, columns[:, 0]
    )
    grad_normed = (full_right_factor(grad_packed, qkv_full) + extra_term).astype(jnp.bfloat16)
    grad_inputs = grad_middle + norm_backward(
        grad_normed.astype(jnp.float32), norm1_gain, first_normal, first_scaled
    )
    grad_windows = grad_inputs.astype(jnp.bfloat16)

    both = jnp.concatenate([block_windows, grad_windows], axis=1)
    arrived = swap_quarters(full_left_factor(window_pick, both).astype(jnp.bfloat16))
    both = full_left_factor(send_pick, arrived).astype(jnp.bfloat16)
    summed = scatter_sums(
        (
            qkv_dgrad,
            proj_dgrad,
            expand_dgrad,
            reduce_dgrad,
            qkv_ugrad,
            proj_ugrad,
            expand_ugrad,
            reduce_ugrad,
        ),
        devices,
    )
    return (
        both[:, :model_width].reshape(tokens.shape),
        both[:, model_width:].reshape(tokens.shape),
        summed[0],
        summed[4].T,
        summed[1],
        summed[5].T,
        summed[2],
        summed[6].T,
        summed[3],
        summed[7].T,
    )


def solution(mesh):
    rows = P(both_axes, None)
    columns = P(None, both_axes)
    image = P("img", "tile", None, None)
    placed = (
        (image,)
        + (rows,) * 4
        + (rows, columns) * 4
        + (P(),) * 9
        + (P("img"), P("img", None), image)
    )

    def step(*arrays):
        return shards(mesh.size, *arrays)

    return jax.shard_map(
        step,
        mesh=mesh,
        in_specs=placed,
        out_specs=(image, image) + (rows, columns) * 4,
        check_vma=False,
    )
```
